32 devices in a mesh: groups: 1, expert: 16 (over z, y, x), tensor: 2 (over core).
Axes of the slice: x: 2, y: 2, z: 4, core: 2. Of those that a mesh axis runs over, the one named last changes fastest.
Arguments:
- hidden_in: bfloat16 [256, 3584], P(('groups', 'expert')), may hold values from -6 to 6
- batch_len: int32 [1], P('groups'), may hold values from 64 to 256
- expert_ids: int32 [256, 8], P(('groups', 'expert')), may hold values from 0 to 15, all different within a row; in each aligned block of 16 rows (0 to 15, 16 to 31, ...) at most 12 rows name the same one
- gate_num: int32 [256, 8], P(('groups', 'expert')), may hold values from 1 to 1024
- w_gate: bfloat16 [16, 3584, 1024], P('expert', None, 'tensor'), may hold values from -0.09375 to 0.09375
- w_up: bfloat16 [16, 3584, 1024], P('expert', None, 'tensor'), may hold values from -0.09375 to 0.09375
- w_down: bfloat16 [16, 1024, 3584], P('expert', 'tensor'), may hold values from -0.1875 to 0.1875
- q_latent: bfloat16 [2, 64, 512], P('groups', 'tensor'), may hold values from -117 to 117
- q_rope: bfloat16 [2, 64, 64], P('groups', 'tensor'), may hold values from -6 to 6
- kv_latent: bfloat16 [2, 2048, 512], P('groups', 'expert'), may hold values from -4 to 4
- kv_rope: bfloat16 [2, 64, 2048], P('groups', None, 'expert'), may hold values from -4 to 4
- ctx_len: int32 [2], P('groups'), may hold values from 1 to 2048, as said below
Outputs:
- moe_out: bfloat16 [256, 3584], P(('groups', 'expert'))
- attn_out: bfloat16 [2, 64, 512], P('groups', 'tensor')
The draws below stay inside these ranges and needn't reach their ends.
Inputs may be any that keep to these rules, and one draw needn't show every extreme that they name: `expert_ids`: each row names 8 different experts; the 16 rows of one index of the expert axis name any one expert at most 12 times. `batch_len`: the live slots are the first ones of the replica. `ctx_len`: the first request's context fills all 2048 positions.
All inputs are finite; a program needn't handle non-finite values.
Results may differ from the reference program's by a relative error of at most 0.0028.
The reference program's roundings to bfloat16 on the way count: a program that leaves them out, or rounds other values in their place, can miss the bound.
Values may be sent and summed in bfloat16 or wider, within the bound.
A program may use at most 64 MiB of HBM per device.

```python
import math
import jax
import jax.numpy as jnp
import numpy as np
from jax import lax

D = 3584
FF = 1024
TOPK = 8
H = 64
LAT = 512
ROPE = 64
TOK_DEV = 16
BATCH = 2
EXPERTS = 16
TOKENS = 256
CAP = 12
CTX = 2048
N_EXPERT = 16


def cache_pair(key):
    base = jax.random.fold_in(key, 71)
    first, second = jax.random.split(base)
    latent = jax.random.truncated_normal(first, -4.0, 4.0, (BATCH, CTX, LAT), jnp.float32)
    rotary = jax.random.truncated_normal(second, -4.0, 4.0, (BATCH, ROPE, CTX), jnp.float32)
    return (latent, rotary)


def draw_kv_latent(key, part):
    return cache_pair(key)[0].astype(jnp.bfloat16)


def draw_kv_rope(key, part):
    return cache_pair(key)[1].astype(jnp.bfloat16)


def draw_ctx_len(key, part):
    lengths = jax.random.randint(jax.random.fold_in(key, 53), (BATCH,), 1, CTX + 1, dtype=jnp.int32)
    first = jnp.arange(BATCH, dtype=jnp.int32) == 0
    return jnp.where(first, CTX, lengths).astype(jnp.int32)


def draw_q_latent(key, part):
    noise = jax.random.truncated_normal(jax.random.fold_in(key, 37), -4.0, 4.0, (BATCH, H, LAT), jnp.float32)
    latent = cache_pair(key)[0]
    head_anchor = latent[:, 0, :] + latent[:, 1, :]
    tail_anchor = latent[:, CTX - 2, :] + latent[:, CTX - 1, :]
    first = (jnp.arange(BATCH, dtype=jnp.int32) == 0)[:, None]
    anchor = jnp.where(first, tail_anchor, head_anchor)
    length_sq = jnp.sum(anchor * anchor, axis=1) + 1.0
    heads = jnp.arange(H, dtype=jnp.int32)
    strength = 250.0 + 150.0 * (heads // 2 % 3).astype(jnp.float32)
    chosen = heads % 2 == 0
    direction = anchor * 192.0 ** 0.5 / length_sq[:, None]
    aligned = strength[None, :, None] * direction[:, None, :]
    mixed = jnp.where(chosen[None, :, None], aligned, noise)
    bound = float(60000 // LAT)
    return jnp.clip(mixed, -bound, bound).astype(jnp.bfloat16)


def touch_ends(drawn, own_key, smallest, top_value):
    dims = drawn.shape
    spot = [jax.random.randint(jax.random.fold_in(own_key, axis), (), 0, dims[axis]) for axis in range(len(dims))]
    drawn = drawn.at[tuple(spot)].set(smallest)
    longest = dims.index(max(dims))
    spot[longest] = (spot[longest] + 1) % dims[longest]
    return drawn.at[tuple(spot)].set(top_value)


def block_levels(own_key, extent, pieces, low, largest):
    def one(axis_at, shards_of):
        draws = jax.random.uniform(jax.random.fold_in(jax.random.fold_in(own_key, 6), axis_at), (shards_of,), jnp.float32, low / len(pieces), largest / len(pieces))
        return jnp.repeat(jnp.exp(draws), extent[axis_at] // shards_of).reshape((-1,) + (1,) * (len(extent) - axis_at - 1))

    factor_of = one(*pieces[0])
    for cut in pieces[1:]:
        factor_of = factor_of * one(*cut)
    return factor_of


def assign_block(stream_key, own, number, rows, count, top, reach, slope):
    order = jax.random.permutation(stream_key, count)
    heavy_load, ordinary = shares(count, rows * top, reach, slope, True), shares(count, rows * top, reach, slope, False)
    places = jnp.arange(count)

    def named(sizes, offset_by):
        used = int((sizes > 0).sum())
        fixed = max(1, used // 4)
        shifted = fixed + (places - fixed + offset_by * (used - fixed)) % max(1, count - fixed)
        return jnp.zeros((count,), jnp.int32).at[order[jnp.where(places < fixed, places, shifted)]].set(jnp.asarray(sizes, jnp.int32))

    sizes = jnp.where(number % 4 == 0, named(heavy_load, number // 4), named(ordinary, number - number // 4 - 1))
    mixed = jax.random.permutation(jax.random.fold_in(own, 3), count)
    donor, taker = mixed[0:count // 2 * 2:2], mixed[1:count // 2 * 2:2]
    margin = jnp.minimum(sizes[donor] - 1, reach - sizes[taker]) // 2
    margin = jnp.where((donor == order[0]) | (taker == order[0]) | (sizes[taker] == 0), 0, jnp.maximum(margin, 0))
    shifted = jax.random.randint(jax.random.fold_in(own, 4), (count // 2,), 0, 1 << 20) % (margin + 1)
    sizes = sizes.at[donor].add(-shifted).at[taker].add(shifted)
    items = jnp.searchsorted(jnp.cumsum(sizes), jnp.arange(rows * top), side="right").astype(jnp.int32)
    listing = items.reshape(top, rows).T
    listing = listing[jax.random.permutation(jax.random.fold_in(own, 1), rows)]
    offset_by = jax.random.randint(jax.random.fold_in(own, 2), (rows, 1), 0, top)
    return jnp.take_along_axis(listing, (jnp.arange(top)[None, :] + offset_by) % top, axis=1)


def shares(count, total, most, skew, full):
    loads = [(1 << 20) // math.isqrt(grade ** skew) + 1 for grade in range(1, count + 1)]
    largest = most if full else min(most, max(-(-total // count), total * loads[0] // sum(loads)))
    least = 1 if total - largest >= count - 1 else 0
    holding, rest = [largest] + [least] * (count - 1), total - largest - least * (count - 1)
    while rest > 0:
        free = [i for i in range(1, count) if holding[i] < largest] or [i for i in range(1, count) if holding[i] < most]
        pool, budget = sum([loads[i] for i in free]), rest
        for i in free:
            more = min(most - holding[i], max(1, budget * loads[i] // pool), rest)
            holding[i] = holding[i] + more
            rest = rest - more
    return np.array(holding)


def gaussian(stream_key, shape, width, reach, cuts=(), kind=jnp.bfloat16):
    values = width * jax.random.normal(stream_key, shape, jnp.float32)
    if cuts:
        values = values * block_levels(stream_key, shape, cuts, -0.22, 0.18)
    return jnp.clip(values, -reach, reach).astype(kind)


def setup_inputs(seed: int = 0, part: int = 0) -> dict:
    key_of = jax.random.split(jax.random.key(seed), 13)
    own_keys = jax.random.split(jax.random.fold_in(key_of[12], part), 13)
    hidden_in = gaussian(own_keys[0], (TOKENS, D), 1.0, 6.0, ((0, 16),))
    batch_len = jax.random.randint(own_keys[1], (1,), TOKENS // 4, TOKENS + 1).astype(jnp.int32)
    expert_ids_keys = jax.random.split(jax.random.fold_in(own_keys[2], 1), TOKENS // TOK_DEV)
    expert_ids_turns = jax.random.permutation(jax.random.fold_in(own_keys[2], 3), TOKENS // TOK_DEV)
    expert_ids = jax.vmap(lambda own, number: assign_block(jax.random.fold_in(own_keys[2], 2), own, number, TOK_DEV, EXPERTS, TOPK, CAP, 2))(expert_ids_keys, expert_ids_turns).reshape((TOKENS, TOPK))
    gate_num = touch_ends(jax.random.randint(own_keys[3], (TOKENS, TOPK), 1, 1025), jax.random.fold_in(own_keys[3], 1), 1, 1024).astype(jnp.int32)
    w_gate = gaussian(key_of[4], (EXPERTS, D, FF), D ** -0.5, 0.09375, ((0, 16), (2, 2)))
    w_up = gaussian(key_of[5], (EXPERTS, D, FF), D ** -0.5, 0.09375, ((0, 16), (2, 2)))
    w_down = gaussian(key_of[6], (EXPERTS, FF, D), FF ** -0.5, 0.1875, ((0, 16), (1, 2)))
    q_latent = draw_q_latent(jax.random.fold_in(jax.random.fold_in(key_of[12], part), 71), part)
    q_rope = gaussian(own_keys[8], (BATCH, H, ROPE), 1.0, 6.0, ((1, 2),))
    kv_latent = draw_kv_latent(jax.random.fold_in(jax.random.fold_in(key_of[12], part), 71), part)
    kv_rope = draw_kv_rope(jax.random.fold_in(jax.random.fold_in(key_of[12], part), 71), part)
    ctx_len = draw_ctx_len(jax.random.fold_in(jax.random.fold_in(key_of[12], part), 71), part)
    return dict(hidden_in=hidden_in, batch_len=batch_len, expert_ids=expert_ids, gate_num=gate_num, w_gate=w_gate, w_up=w_up, w_down=w_down, q_latent=q_latent, q_rope=q_rope, kv_latent=kv_latent, kv_rope=kv_rope, ctx_len=ctx_len)


gate_denominator = 1024.0
softmax_scale = 192.0 ** -0.5


def reference(hidden_in, batch_len, expert_ids, gate_num, w_gate, w_up, w_down, q_latent, q_rope, kv_latent, kv_rope, ctx_len):
    live = jnp.arange(TOKENS, dtype=jnp.int32) < batch_len[0]
    flat_expert = expert_ids.reshape(-1)
    token_of = jnp.arange(TOKENS * TOPK, dtype=jnp.int32) // TOPK
    live_pick = live[token_of]
    weight = jnp.where(live_pick, gate_num.reshape(-1).astype(jnp.float32) / gate_denominator, 0.0)
    rows_most = N_EXPERT * CAP

    def one_expert(total, index):
        match = (flat_expert == index) & live_pick
        picked = jnp.nonzero(match, size=rows_most, fill_value=0)[0].astype(jnp.int32)
        valid = jnp.arange(rows_most, dtype=jnp.int32) < jnp.sum(match.astype(jnp.int32))
        tokens = token_of[picked]
        rows = hidden_in[tokens]
        gate = jnp.dot(rows, w_gate[index], preferred_element_type=jnp.float32)
        upper = jnp.dot(rows, w_up[index], preferred_element_type=jnp.float32)
        hidden = (jax.nn.silu(gate) * upper).astype(jnp.bfloat16)
        value = jnp.dot(hidden, w_down[index], preferred_element_type=jnp.float32).astype(jnp.bfloat16)
        value = lax.optimization_barrier(value).astype(jnp.float32)
        scaled = value * jnp.where(valid, weight[picked], 0.0)[:, None]
        return total.at[tokens].add(scaled), None

    start = jnp.zeros((TOKENS, D), jnp.float32)
    summed, unused = lax.scan(one_expert, start, jnp.arange(EXPERTS, dtype=jnp.int32))
    moe_out = summed.astype(jnp.bfloat16)

    scores = jnp.einsum("bhl,bpl->bhp", q_latent.astype(jnp.float32), kv_latent.astype(jnp.float32))
    scores = scores + jnp.einsum("bhr,brp->bhp", q_rope.astype(jnp.float32), kv_rope.astype(jnp.float32))
    scores = scores * softmax_scale
    valid_pos = jnp.arange(CTX, dtype=jnp.int32)[None, :] < ctx_len[:, None]
    scores = jnp.where(valid_pos[:, None, :], scores, -1e30)
    top = jnp.max(scores, axis=2, keepdims=True)
    probs = jnp.where(valid_pos[:, None, :], jnp.exp(scores - top), 0.0)
    total = jnp.sum(probs, axis=2, keepdims=True)
    probs_bf = lax.optimization_barrier(probs.astype(jnp.bfloat16)).astype(jnp.float32)
    weighted = jnp.einsum("bhp,bpl->bhl", probs_bf, kv_latent.astype(jnp.float32))
    attn_out = (weighted / total).astype(jnp.bfloat16)
    return moe_out, attn_out
```

```python
import functools

import jax
import jax.numpy as jnp
from jax import lax
from jax.experimental import pallas as pl
from jax.experimental.pallas import tpu as pltpu
from jax.sharding import PartitionSpec as P

gate_denominator = 1024.0
softmax_scale = 192.0 ** (-0.5)
LANES = 128
SUB = 8
F32 = jnp.float32
BF16 = jnp.bfloat16


def iota(shape, dim):
    return lax.broadcasted_iota(jnp.int32, shape, dim)


def remote(src, dst, send, recv, **where):
    return pltpu.make_async_remote_copy(
        src_ref=src,
        dst_ref=dst,
        send_sem=send,
        recv_sem=recv,
        device_id=where,
        device_id_type=pl.DeviceIdType.MESH,
    )


def kernel(
    n,
    full,
    fold,
    chunks,
    x_hbm,
    blen,
    ids,
    gnum,
    wg_hbm,
    wu_hbm,
    wd_hbm,
    ql,
    qr,
    kvl_hbm,
    kvr_hbm,
    clen,
    moe_out,
    attn_out,
    xb,
    xp,
    wg,
    wu,
    wd,
    kvl,
    kvr,
    hid,
    val,
    ret,
    aps,
    apr,
    ares,
    ob,
    op,
    local_sem,
    col_recv,
    x_recv,
    y_recv,
    d_recv,
    send_sem,
    recv_sem,
):
    me = lax.axis_index("expert")
    core = lax.axis_index("tensor")
    other = 1 - core
    rows, width = x_hbm.shape
    half = width // 2
    quarter = half // 2
    topk = ids.shape[1]
    outer = n // 4
    tokens = n * rows
    batch, heads, lat = ql.shape
    mine = pl.ds(pl.multiple_of(core * half, LANES), half)
    theirs = pl.ds(pl.multiple_of(other * half, LANES), half)

    x_load = pltpu.make_async_copy(
        x_hbm.at[:, mine], xb.at[me, :, pl.ds(LANES, half)], local_sem.at[0]
    )
    x_load.start()
    kv_loads = [
        pltpu.make_async_copy(kvl_hbm, kvl, local_sem.at[1]),
        pltpu.make_async_copy(kvr_hbm, kvr, local_sem.at[2]),
    ]
    for copy in kv_loads:
        copy.start()
    mine_rows = pl.ds(pl.multiple_of(core * half, LANES), half)
    their_rows = pl.ds(pl.multiple_of(other * half, LANES), half)
    w_loads = [
        pltpu.make_async_copy(wg_hbm.at[0, mine_rows], wg.at[0], local_sem.at[3]),
        pltpu.make_async_copy(wu_hbm.at[0, mine_rows], wu.at[0], local_sem.at[4]),
        pltpu.make_async_copy(wg_hbm.at[0, their_rows], wg.at[1], local_sem.at[5]),
        pltpu.make_async_copy(wu_hbm.at[0, their_rows], wu.at[1], local_sem.at[6]),
        pltpu.make_async_copy(wd_hbm.at[0, :, mine], wd.at[core], local_sem.at[7]),
    ]

    barrier = pltpu.get_barrier_semaphore()

    def greet(step, carry):
        pl.semaphore_signal(
            barrier,
            inc=1,
            device_id={"expert": lax.rem(me + step, n)},
            device_id_type=pl.DeviceIdType.MESH,
        )
        return carry

    lax.fori_loop(1, n, greet, 0)
    pl.semaphore_signal(
        barrier, inc=1, device_id={"tensor": other}, device_id_type=pl.DeviceIdType.MESH
    )

    live = (me * rows + iota((rows, LANES), 0)) < blen[0]
    lane = iota((rows, LANES), 1)
    named = jnp.zeros((rows, LANES), F32)
    gates = jnp.zeros((rows, LANES), jnp.int32)
    for k in range(topk):
        hit = (ids[:, k : k + 1] == lane) & live
        named = named + jnp.where(hit, 1.0, 0.0)
        gates = gates + jnp.where(hit, gnum[:, k : k + 1], 0)
    below = jnp.where(iota((rows, rows), 1) < iota((rows, rows), 0), 1.0, 0.0).astype(BF16)
    rank = jnp.dot(below, named.astype(BF16), preferred_element_type=F32)
    code = jnp.where(named > 0.5, rank + 1.0, 0.0)
    xb[me, :, 0:LANES] = code.astype(BF16)

    x_load.wait()
    pl.semaphore_wait(barrier, n)

    bit_x = lax.rem(me, 2)
    bit_y = lax.rem(me // 2, 2)
    plane = me - 2 * bit_y - bit_x
    spot = 2 * bit_y + bit_x
    group = me // 4
    x_side = me + 1 - 2 * bit_x
    y_side = me + 2 - 4 * bit_y
    x_spot = spot + 1 - 2 * bit_x
    y_spot = spot + 2 - 4 * bit_y
    d_spot = 3 - spot
    cuts = (pl.ds(0, LANES + quarter), pl.ds(LANES + quarter, quarter))
    feats = (pl.ds(LANES, quarter), pl.ds(LANES + quarter, quarter))
    lands = (pl.ds(0, quarter), pl.ds(quarter, quarter))

    def block_of(step, place):
        return lax.rem(group - step + outer, outer) * 4 + place

    def to_core(block, h):
        remote(
            xb.at[block, :, feats[h]],
            xp.at[block, :, lands[h]],
            send_sem.at[0],
            recv_sem.at[0],
            tensor=other,
        ).start()

    def to_x(block, h, recv):
        part = xb.at[block, :, cuts[h]]
        remote(part, part, send_sem.at[1], recv, expert=x_side).start()

    def to_y(block, h, recv):
        part = xb.at[block, :, cuts[h]]
        remote(part, part, send_sem.at[2], recv, expert=y_side).start()

    def landed(block, h, recv):
        part = xb.at[block, :, cuts[h]]
        remote(part, part, send_sem.at[3], recv, expert=x_side).wait_recv()

    for h in range(2):
        to_x(me, h, x_recv.at[0, h])
        to_y(me, h, y_recv.at[0, h])
        for step in range(1, outer):
            part = xb.at[me, :, cuts[h]]
            remote(
                part,
                part,
                send_sem.at[3],
                col_recv.at[step, h],
                expert=lax.rem(group + step, outer) * 4 + spot,
            ).start()
    for h in range(2):
        to_core(me, h)
    for copy in w_loads:
        copy.start()
    w_swap = remote(
        wd_hbm.at[0, :, theirs], wd.at[core], send_sem.at[4], recv_sem.at[1], tensor=other
    )
    w_swap.start()

    for copy in kv_loads:
        copy.wait()
    positions = kvl.shape[1]
    where_p = me * positions + iota((heads, positions), 1)
    parts = lat * SUB * chunks // (batch * heads * lat)
    part_w = lat // parts
    per_batch = heads // SUB
    for b in range(batch):
        valid = where_p < clen[b]
        scores = lax.dot_general(
            ql[b], kvl[b], (((1,), (1,)), ((), ())), preferred_element_type=F32
        )
        scores = scores + jnp.dot(qr[b], kvr[b], preferred_element_type=F32)
        scores = jnp.where(valid, scores * softmax_scale, -1e30)
        peak = jnp.max(scores, axis=1, keepdims=True)
        probs = jnp.where(valid, jnp.exp(scores - peak), 0.0)
        total = jnp.sum(probs, axis=1, keepdims=True)
        weighted = jnp.dot(probs.astype(BF16), kvl[b], preferred_element_type=F32)
        both = jnp.where(iota((heads, LANES), 1) < LANES // 2, peak, total)
        for g in range(per_batch):
            rs = slice(g * SUB, (g + 1) * SUB)
            for c in range(parts):
                at = (b * per_batch + g) * parts + c
                aps[at, :, 0:part_w] = weighted[rs, c * part_w : (c + 1) * part_w]
                aps[at, :, part_w : part_w + LANES] = both[rs]

    def share(step, carry):
        dest = lax.rem(me + step, n)

        @pl.when(dest < chunks)
        def _():
            remote(
                aps.at[dest], apr.at[me], send_sem.at[5], recv_sem.at[2], expert=dest
            ).start()

        return carry

    lax.fori_loop(1, n, share, 0)

    for step in range(outer):
        if step + 1 < outer:
            block = block_of(step + 1, spot)
            for h in range(2):
                landed(block, h, col_recv.at[step + 1, h])
                to_x(block, h, x_recv.at[step + 1, h])
                to_y(block, h, y_recv.at[step + 1, h])
                to_core(block, h)
        from_x, from_y = block_of(step, x_spot), block_of(step, y_spot)
        landed(from_x, 0, x_recv.at[step, 0])
        to_y(from_x, 0, d_recv.at[step, 0])
        to_core(from_x, 0)
        landed(from_y, 0, y_recv.at[step, 0])
        to_core(from_y, 0)
        landed(from_y, 1, y_recv.at[step, 1])
        to_x(from_y, 1, d_recv.at[step, 1])
        to_core(from_y, 1)
        landed(from_x, 1, x_recv.at[step, 1])
        to_core(from_x, 1)
    for step in range(outer):
        block = block_of(step, d_spot)
        for h in range(2):
            landed(block, h, d_recv.at[step, h])
            to_core(block, h)

    seen = jnp.where(iota((SUB, LANES), 1) == me, 1.0, 0.0).astype(BF16)
    codes = xb[:, :, 0:LANES].reshape(tokens, LANES)
    code_row = lax.dot_general(
        seen, codes, (((1,), (1,)), ((), ())), preferred_element_type=F32
    )[0:1]
    groups = full + fold
    packs = []
    for g in range(groups):
        r = iota((n * SUB, tokens), 0)
        j = r % SUB
        slot = g * SUB + (j if g < full else j % (SUB // 2))
        same = (r // SUB) == (iota((n * SUB, tokens), 1) // rows)
        hit = same & (code_row == (slot + 1).astype(F32))
        packs.append(jnp.where(hit, 1.0, 0.0).astype(BF16))
    pack = jnp.concatenate(packs, axis=0) if groups > 1 else packs[0]

    for copy in w_loads[:4]:
        copy.wait()
    x_own = xb[:, :, LANES:].reshape(tokens, half)
    gate = jnp.dot(x_own, wg[0], preferred_element_type=F32)
    upper = jnp.dot(x_own, wu[0], preferred_element_type=F32)
    remote(xp, xp, send_sem.at[0], recv_sem.at[0], tensor=other).wait_recv()
    x_other = xp[...].reshape(tokens, half)
    gate = gate + jnp.dot(x_other, wg[1], preferred_element_type=F32)
    upper = upper + jnp.dot(x_other, wu[1], preferred_element_type=F32)
    hidden = (gate / (1.0 + jnp.exp(-gate)) * upper).astype(BF16)
    hid[core] = hidden
    h_swap = remote(hid.at[core], hid.at[core], send_sem.at[6], recv_sem.at[3], tensor=other)
    h_swap.start()

    @pl.when(me < chunks)
    def _():
        remote(
            apr.at[pl.ds(0, n - 1)],
            apr.at[pl.ds(0, n - 1)],
            send_sem.at[5],
            recv_sem.at[2],
            expert=x_side,
        ).wait_recv()
        apr[me] = aps[me]
        peaks = apr[:, :, part_w : part_w + 1]
        totals = apr[:, :, part_w + LANES // 2 : part_w + LANES // 2 + 1]
        top = jnp.max(peaks, axis=0, keepdims=True)
        scale = jnp.exp(peaks - top)
        total = jnp.sum(totals * scale, axis=0)
        joined = jnp.sum(apr[:, :, 0:part_w] * scale, axis=0)
        ares[me] = (joined / total).astype(BF16)

        def tell(step, carry):
            remote(
                ares.at[me],
                ares.at[me],
                send_sem.at[7],
                recv_sem.at[4],
                expert=lax.rem(me + step, n),
            ).start()
            return carry

        lax.fori_loop(1, n, tell, 0)

    w_loads[4].wait()
    w_swap.wait_recv()
    own_packed = jnp.dot(pack, hid[core], preferred_element_type=F32).astype(BF16)
    value = jnp.dot(own_packed, wd[core], preferred_element_type=F32)
    h_swap.wait_recv()
    their_packed = jnp.dot(pack, hid[other], preferred_element_type=F32).astype(BF16)
    value = (value + jnp.dot(their_packed, wd[other], preferred_element_type=F32)).astype(BF16)
    left, right = value[:, :quarter], value[:, quarter:]
    for g in range(full):
        rs = slice(g * n * SUB, (g + 1) * n * SUB)
        val[:, 2 * g] = left[rs].reshape(n, SUB, quarter)
        val[:, 2 * g + 1] = right[rs].reshape(n, SUB, quarter)
    if fold:
        rs = slice(full * n * SUB, (full + 1) * n * SUB)
        low = iota((n * SUB, quarter), 0) % SUB < SUB // 2
        val[:, 2 * full] = jnp.where(low, left[rs], right[rs]).reshape(n, SUB, quarter)

    def give(step, carry):
        dest = lax.rem(me + step, n)
        remote(val.at[dest], ret.at[me], send_sem.at[8], recv_sem.at[5], expert=dest).start()
        return carry

    lax.fori_loop(1, n, give, 0)
    ret[me] = val[me]

    high = gates // 16 * 16
    spread_in = jnp.concatenate(
        [high.astype(F32), (gates - high).astype(F32), code], axis=0
    ).astype(BF16)
    spot_of = jnp.where(
        iota((LANES, n * SUB), 0) == iota((LANES, n * SUB), 1) // SUB, 1.0, 0.0
    ).astype(BF16)
    spread = jnp.dot(spread_in, spot_of, preferred_element_type=F32)
    weights = spread[: 2 * rows]
    codes_r = spread[2 * rows :]
    codes_r = jnp.concatenate([codes_r, codes_r], axis=0)
    j = iota((2 * rows, n * SUB), 1) % SUB
    mats = []
    for g in range(full):
        hit = codes_r == (g * SUB + j + 1).astype(F32)
        mats.append(jnp.where(hit, weights, 0.0).astype(BF16))
    if fold:
        hit = codes_r == (full * SUB + j % (SUB // 2) + 1).astype(F32)
        for low in (True, False):
            side = (j < SUB // 2) if low else (j >= SUB // 2)
            mats.append(jnp.where(hit & side, weights, 0.0).astype(BF16))

    @pl.when(me < chunks)
    def _():
        part = ares.at[pl.ds(0, chunks - 1)]
        remote(part, part, send_sem.at[7], recv_sem.at[4], expert=x_side).wait_recv()

    if chunks < n:

        @pl.when(me >= chunks)
        def _():
            remote(ares, ares, send_sem.at[7], recv_sem.at[4], expert=x_side).wait_recv()

    for b in range(batch):
        for g in range(per_batch):
            for c in range(parts):
                at = (b * per_batch + g) * parts + c
                attn_out[b, g * SUB : (g + 1) * SUB, c * part_w : (c + 1) * part_w] = ares[at]

    remote(xp, xp, send_sem.at[0], recv_sem.at[0], tensor=other).wait_send()
    for sem in (1, 2):
        part = xb.at[pl.ds(0, outer)]
        remote(part, part, send_sem.at[sem], recv_sem.at[0], expert=x_side).wait_send()
    for h in range(outer):
        part = xb.at[h, :, cuts[0]]
        remote(part, part, send_sem.at[2], recv_sem.at[0], expert=x_side).wait_send()
        part = xb.at[h, :, cuts[1]]
        remote(part, part, send_sem.at[1], recv_sem.at[0], expert=x_side).wait_send()
    part = xb.at[pl.ds(0, outer - 1)]
    remote(part, part, send_sem.at[3], recv_sem.at[0], expert=x_side).wait_send()
    w_swap.wait_send()
    h_swap.wait_send()

    sent = chunks - jnp.where(me < chunks, 1, 0)

    def drain(step, carry):
        remote(aps.at[0], apr.at[0], send_sem.at[5], recv_sem.at[2], expert=x_side).wait_send()
        return carry

    lax.fori_loop(0, sent, drain, 0)

    @pl.when(me < chunks)
    def _():
        def drain_result(step, carry):
            remote(
                ares.at[0], ares.at[0], send_sem.at[7], recv_sem.at[4], expert=x_side
            ).wait_send()
            return carry

        lax.fori_loop(1, n, drain_result, 0)

    part = ret.at[pl.ds(0, n - 1)]
    remote(part, part, send_sem.at[8], recv_sem.at[5], expert=x_side).wait_recv()
    lo = jnp.zeros((2 * rows, quarter), F32)
    hi = jnp.zeros((2 * rows, quarter), F32)
    for g in range(full):
        lo = lo + jnp.dot(
            mats[g], ret[:, 2 * g].reshape(n * SUB, quarter), preferred_element_type=F32
        )
        hi = hi + jnp.dot(
            mats[g], ret[:, 2 * g + 1].reshape(n * SUB, quarter), preferred_element_type=F32
        )
    if fold:
        last = ret[:, 2 * full].reshape(n * SUB, quarter)
        lo = lo + jnp.dot(mats[full], last, preferred_element_type=F32)
        hi = hi + jnp.dot(mats[full + 1], last, preferred_element_type=F32)
    ob[:, :quarter] = ((lo[:rows] + lo[rows:]) / gate_denominator).astype(BF16)
    ob[:, quarter:] = ((hi[:rows] + hi[rows:]) / gate_denominator).astype(BF16)
    o_swap = remote(ob, op, send_sem.at[9], recv_sem.at[6], tensor=other)
    o_swap.start()
    moe_out[:, mine] = ob[...]
    remote(part, part, send_sem.at[8], recv_sem.at[5], expert=x_side).wait_send()
    o_swap.wait()
    moe_out[:, theirs] = op[...]


def local(
    hidden_in,
    batch_len,
    expert_ids,
    gate_num,
    w_gate,
    w_up,
    w_down,
    q_latent,
    q_rope,
    kv_latent,
    kv_rope,
    ctx_len,
):
    n = lax.axis_size("expert")
    rows, width = hidden_in.shape
    topk = expert_ids.shape[1]
    capacity = min(rows, max(2, 3 * rows * topk // (2 * n)))
    rest = capacity % SUB
    full = capacity // SUB + (1 if rest > SUB // 2 else 0)
    fold = 1 if 0 < rest <= SUB // 2 else 0
    half = width // 2
    hidden = w_gate.shape[2]
    batch, heads, lat = q_latent.shape
    row_groups = batch * heads // SUB
    chunks = row_groups * min(max(1, n // row_groups), lat // LANES)
    part_w = lat * row_groups // chunks
    parts_v = 2 * full + fold
    outer = n // 4
    anywhere = pl.BlockSpec(memory_space=pl.ANY)
    vmem = pl.BlockSpec(memory_space=pltpu.VMEM)
    smem = pl.BlockSpec(memory_space=pltpu.SMEM)
    return pl.pallas_call(
        functools.partial(kernel, n, full, fold, chunks),
        out_shape=(
            jax.ShapeDtypeStruct((rows, width), BF16),
            jax.ShapeDtypeStruct((batch, heads, lat), BF16),
        ),
        in_specs=[
            anywhere,
            smem,
            vmem,
            vmem,
            anywhere,
            anywhere,
            anywhere,
            vmem,
            vmem,
            anywhere,
            anywhere,
            smem,
        ],
        out_specs=(vmem, vmem),
        scratch_shapes=[
            pltpu.VMEM((n, rows, LANES + half), BF16),
            pltpu.VMEM((n, rows, half), BF16),
            pltpu.VMEM((2, half, hidden), BF16),
            pltpu.VMEM((2, half, hidden), BF16),
            pltpu.VMEM((2, hidden, half), BF16),
            pltpu.VMEM(kv_latent.shape, BF16),
            pltpu.VMEM(kv_rope.shape, BF16),
            pltpu.VMEM((2, n * rows, hidden), BF16),
            pltpu.VMEM((n, parts_v, SUB, half // 2), BF16),
            pltpu.VMEM((n, parts_v, SUB, half // 2), BF16),
            pltpu.VMEM((chunks, SUB, part_w + LANES), F32),
            pltpu.VMEM((n, SUB, part_w + LANES), F32),
            pltpu.VMEM((chunks, SUB, part_w), BF16),
            pltpu.VMEM((rows, half), BF16),
            pltpu.VMEM((rows, half), BF16),
            pltpu.SemaphoreType.DMA((8,)),
            pltpu.SemaphoreType.DMA((outer, 2)),
            pltpu.SemaphoreType.DMA((outer, 2)),
            pltpu.SemaphoreType.DMA((outer, 2)),
            pltpu.SemaphoreType.DMA((outer, 2)),
            pltpu.SemaphoreType.DMA((10,)),
            pltpu.SemaphoreType.DMA((7,)),
        ],
        compiler_params=pltpu.CompilerParams(
            collective_id=0, has_side_effects=True, vmem_limit_bytes=60 * 1024 * 1024
        ),
    )(
        hidden_in,
        batch_len,
        expert_ids,
        gate_num,
        w_gate,
        w_up,
        w_down,
        q_latent,
        q_rope,
        kv_latent,
        kv_rope,
        ctx_len,
    )


def solution(mesh):
    return jax.shard_map(
        local,
        mesh=mesh,
        in_specs=(
            P(("groups", "expert"), None),
            P("groups"),
            P(("groups", "expert"), None),
            P(("groups", "expert"), None),
            P("expert", None, "tensor"),
            P("expert", None, "tensor"),
            P("expert", "tensor", None),
            P("groups", "tensor", None),
            P("groups", "tensor", None),
            P("groups", "expert", None),
            P("groups", None, "expert"),
            P("groups"),
        ),
        out_specs=(P(("groups", "expert"), None), P("groups", "tensor", None)),
        check_vma=False,
    )
```

```python
import functools

import jax
import jax.numpy as jnp
from jax import lax
from jax.experimental import pallas as pl
from jax.experimental.pallas import tpu as pltpu
from jax.sharding import PartitionSpec as P

gate_denominator = 1024.0
softmax_scale = 192.0 ** (-0.5)
LANES = 128
SUB = 8
F32 = jnp.float32
BF16 = jnp.bfloat16


def iota(shape, dim):
    return lax.broadcasted_iota(jnp.int32, shape, dim)


def remote(src, dst, send, recv, **where):
    return pltpu.make_async_remote_copy(
        src_ref=src,
        dst_ref=dst,
        send_sem=send,
        recv_sem=recv,
        device_id=where,
        device_id_type=pl.DeviceIdType.MESH,
    )


def kernel(
    n,
    full,
    fold,
    chunks,
    x_hbm,
    blen,
    ids,
    gnum,
    wg_hbm,
    wu_hbm,
    wd_hbm,
    ql,
    qr,
    kvl_hbm,
    kvr_hbm,
    clen,
    moe_out,
    attn_out,
    xb,
    xp,
    wg,
    wu,
    wd,
    kvl,
    kvr,
    hid,
    val,
    ret,
    aps,
    apr,
    ares,
    ob,
    op,
    local_sem,
    col_recv,
    x_recv,
    y_recv,
    d_recv,
    send_sem,
    recv_sem,
):
    me = lax.axis_index("expert")
    core = lax.axis_index("tensor")
    other = 1 - core
    rows, width = x_hbm.shape
    half = width // 2
    quarter = half // 2
    topk = ids.shape[0]
    outer = n // 4
    tokens = n * rows
    batch, heads, lat = ql.shape
    mine = pl.ds(pl.multiple_of(core * half, LANES), half)
    theirs = pl.ds(pl.multiple_of(other * half, LANES), half)

    order = [0] + sorted(range(1, outer), key=lambda step: -min(step, outer - step))
    early = (outer + 1) // 2
    stages = (order[:early], order[early:])

    x_load = pltpu.make_async_copy(
        x_hbm.at[:, mine], xb.at[me, :, pl.ds(LANES, half)], local_sem.at[0]
    )
    x_load.start()
    kv_loads = [
        pltpu.make_async_copy(kvl_hbm, kvl, local_sem.at[1]),
        pltpu.make_async_copy(kvr_hbm, kvr, local_sem.at[2]),
    ]
    for copy in kv_loads:
        copy.start()
    mine_rows = pl.ds(pl.multiple_of(core * half, LANES), half)
    their_rows = pl.ds(pl.multiple_of(other * half, LANES), half)
    w_loads = [
        pltpu.make_async_copy(wg_hbm.at[0, mine_rows], wg.at[0], local_sem.at[3]),
        pltpu.make_async_copy(wu_hbm.at[0, mine_rows], wu.at[0], local_sem.at[4]),
        pltpu.make_async_copy(wg_hbm.at[0, their_rows], wg.at[1], local_sem.at[5]),
        pltpu.make_async_copy(wu_hbm.at[0, their_rows], wu.at[1], local_sem.at[6]),
        pltpu.make_async_copy(wd_hbm.at[0, :, mine], wd.at[core], local_sem.at[7]),
    ]

    for copy in w_loads:
        copy.start()

    barrier = pltpu.get_barrier_semaphore()

    def greet(step, carry):
        pl.semaphore_signal(
            barrier,
            inc=1,
            device_id={"expert": lax.rem(me + step, n)},
            device_id_type=pl.DeviceIdType.MESH,
        )
        return carry

    lax.fori_loop(1, n, greet, 0)
    pl.semaphore_signal(
        barrier, inc=1, device_id={"tensor": other}, device_id_type=pl.DeviceIdType.MESH
    )

    live = (me * rows + iota((LANES, rows), 1)) < blen[0]
    expert = iota((LANES, rows), 0)
    named = jnp.zeros((LANES, rows), F32)
    gates = jnp.zeros((LANES, rows), jnp.int32)
    for k in range(topk):
        hit = (ids[k : k + 1, :] == expert) & live
        named = named + jnp.where(hit, 1.0, 0.0)
        gates = gates + jnp.where(hit, gnum[k : k + 1, :], 0)
    high = gates // 16 * 16
    turn = (((1,), (1,)), ((), ()))
    row, col = iota((rows, rows), 0), iota((rows, rows), 1)
    below = jnp.where(col < row, 1.0, 0.0).astype(BF16)
    same_row = jnp.where(col == row, 1.0, 0.0).astype(BF16)

    def turned(left, right):
        return lax.dot_general(left, right.astype(BF16), turn, preferred_element_type=F32)

    code = jnp.where(turned(same_row, named) > 0.5, turned(below, named) + 1.0, 0.0)
    gate_high = turned(same_row, high.astype(F32))
    gate_low = turned(same_row, (gates - high).astype(F32))
    xb[me, :, 0:LANES] = code.astype(BF16)

    x_load.wait()
    pl.semaphore_wait(barrier, n)

    bit_x = lax.rem(me, 2)
    bit_y = lax.rem(me // 2, 2)
    plane = me - 2 * bit_y - bit_x
    spot = 2 * bit_y + bit_x
    group = me // 4
    x_side = me + 1 - 2 * bit_x
    y_side = me + 2 - 4 * bit_y
    x_spot = spot + 1 - 2 * bit_x
    y_spot = spot + 2 - 4 * bit_y
    d_spot = 3 - spot
    cuts = (pl.ds(0, LANES + quarter), pl.ds(LANES + quarter, quarter))
    feats = (pl.ds(LANES, quarter), pl.ds(LANES + quarter, quarter))
    lands = (pl.ds(0, quarter), pl.ds(quarter, quarter))

    def block_of(step, place):
        return lax.rem(group - step + outer, outer) * 4 + place

    def to_core(block, h, stage):
        remote(
            xb.at[block, :, feats[h]],
            xp.at[block, :, lands[h]],
            send_sem.at[0],
            recv_sem.at[7 + stage],
            tensor=other,
        ).start()

    def to_x(block, h, recv):
        part = xb.at[block, :, cuts[h]]
        remote(part, part, send_sem.at[1], recv, expert=x_side).start()

    def to_y(block, h, recv):
        part = xb.at[block, :, cuts[h]]
        remote(part, part, send_sem.at[2], recv, expert=y_side).start()

    def landed(block, h, recv):
        part = xb.at[block, :, cuts[h]]
        remote(part, part, send_sem.at[3], recv, expert=x_side).wait_recv()

    for h in range(2):
        to_x(me, h, x_recv.at[0, h])
        to_y(me, h, y_recv.at[0, h])
        for step in order[1:]:
            part = xb.at[me, :, cuts[h]]
            remote(
                part,
                part,
                send_sem.at[3],
                col_recv.at[step, h],
                expert=lax.rem(group + step, outer) * 4 + spot,
            ).start()
    for h in range(2):
        to_core(me, h, 0)
    w_swap = remote(
        wd_hbm.at[0, :, theirs], wd.at[core], send_sem.at[4], recv_sem.at[1], tensor=other
    )
    w_swap.start()

    for copy in kv_loads:
        copy.wait()
    positions = kvl.shape[1]
    where_p = me * positions + iota((heads, positions), 1)
    parts = lat * SUB * chunks // (batch * heads * lat)
    part_w = lat // parts
    per_batch = heads // SUB
    for b in range(batch):
        valid = where_p < clen[b]
        scores = lax.dot_general(
            ql[b], kvl[b], (((1,), (1,)), ((), ())), preferred_element_type=F32
        )
        scores = scores + jnp.dot(qr[b], kvr[b], preferred_element_type=F32)
        scores = jnp.where(valid, scores * softmax_scale, -1e30)
        peak = jnp.max(scores, axis=1, keepdims=True)
        probs = jnp.where(valid, jnp.exp(scores - peak), 0.0)
        total = jnp.sum(probs, axis=1, keepdims=True)
        weighted = jnp.dot(probs.astype(BF16), kvl[b], preferred_element_type=F32)
        both = jnp.where(iota((heads, LANES), 1) < LANES // 2, peak, total)
        for g in range(per_batch):
            rs = slice(g * SUB, (g + 1) * SUB)
            for c in range(parts):
                at = (b * per_batch + g) * parts + c
                aps[at, :, 0:part_w] = weighted[rs, c * part_w : (c + 1) * part_w]
                aps[at, :, part_w : part_w + LANES] = both[rs]

    def across(stage):
        for step in stages[stage]:
            block = block_of(step, d_spot)
            for h in range(2):
                landed(block, h, d_recv.at[step, h])
                to_core(block, h, stage)

    for at, step in enumerate(order):
        if at + 1 < outer:
            ahead = order[at + 1]
            block = block_of(ahead, spot)
            for h in range(2):
                landed(block, h, col_recv.at[ahead, h])
                to_x(block, h, x_recv.at[ahead, h])
                to_y(block, h, y_recv.at[ahead, h])
                to_core(block, h, 0 if at + 1 < early else 1)
        stage = 0 if at < early else 1
        from_x, from_y = block_of(step, x_spot), block_of(step, y_spot)
        landed(from_x, 0, x_recv.at[step, 0])
        to_y(from_x, 0, d_recv.at[step, 0])
        to_core(from_x, 0, stage)
        landed(from_y, 0, y_recv.at[step, 0])
        to_core(from_y, 0, stage)
        landed(from_y, 1, y_recv.at[step, 1])
        to_x(from_y, 1, d_recv.at[step, 1])
        to_core(from_y, 1, stage)
        landed(from_x, 1, x_recv.at[step, 1])
        to_core(from_x, 1, stage)
        if at + 2 == outer:
            across(0)

    def share(step, carry):
        dest = lax.rem(me + step, n)

        @pl.when(dest < chunks)
        def _():
            remote(
                aps.at[dest], apr.at[me], send_sem.at[5], recv_sem.at[2], expert=dest
            ).start()

        return carry

    lax.fori_loop(1, n, share, 0)

    groups = full + fold

    def experts(stage, join):
        steps = stages[stage]
        blocks = [pl.ds(block_of(step, 0), 4) for step in steps]
        count = len(steps) * 4

        def taken(ref, cols, size):
            return jnp.concatenate(
                [ref[block, :, cols].reshape(4 * rows, size) for block in blocks], axis=0
            )

        seen = jnp.where(iota((SUB, LANES), 1) == me, 1.0, 0.0).astype(BF16)
        codes = taken(xb, pl.ds(0, LANES), LANES)
        code_row = lax.dot_general(
            seen, codes, (((1,), (1,)), ((), ())), preferred_element_type=F32
        )[0:1]
        shape = (count * SUB, count * rows)
        r = iota(shape, 0)
        j = r % SUB
        same = (r // SUB) == (iota(shape, 1) // rows)
        packs = []
        for g in range(groups):
            slot = g * SUB + (j if g < full else j % (SUB // 2))
            hit = same & (code_row == (slot + 1).astype(F32))
            packs.append(jnp.where(hit, 1.0, 0.0).astype(BF16))
        pack = jnp.concatenate(packs, axis=0) if groups > 1 else packs[0]

        if stage == 0:
            for copy in w_loads[:4]:
                copy.wait()
        x_own = taken(xb, pl.ds(LANES, half), half)
        gate = jnp.dot(x_own, wg[0], preferred_element_type=F32)
        upper = jnp.dot(x_own, wu[0], preferred_element_type=F32)
        arrived = xp.at[pl.ds(0, count)]
        remote(
            arrived, arrived, send_sem.at[0], recv_sem.at[7 + stage], tensor=other
        ).wait_recv()
        x_other = taken(xp, pl.ds(0, half), half)
        gate = gate + jnp.dot(x_other, wg[1], preferred_element_type=F32)
        upper = upper + jnp.dot(x_other, wu[1], preferred_element_type=F32)
        hidden = (gate / (1.0 + jnp.exp(-gate)) * upper).astype(BF16)
        span = pl.ds(stage * early * 4 * rows, count * rows)
        hid[core, span] = hidden
        mine_hid = hid.at[core, span]
        sems = ((6, 3), (10, 9))[stage]
        swap = remote(mine_hid, mine_hid, send_sem.at[sems[0]], recv_sem.at[sems[1]], tensor=other)
        swap.start()

        if stage == 0:
            w_loads[4].wait()
            w_swap.wait_recv()
        own_packed = jnp.dot(pack, hid[core, span], preferred_element_type=F32).astype(BF16)
        value = jnp.dot(own_packed, wd[core], preferred_element_type=F32)
        swap.wait_recv()
        their_packed = jnp.dot(pack, hid[other, span], preferred_element_type=F32).astype(BF16)
        value = (value + jnp.dot(their_packed, wd[other], preferred_element_type=F32)).astype(BF16)
        left, right = value[:, :quarter], value[:, quarter:]
        each = 4 * SUB
        for g in range(groups):
            for i, block in enumerate(blocks):
                at = g * count * SUB + i * each
                one, two = left[at : at + each], right[at : at + each]
                if g < full:
                    val[block, 2 * g] = one.reshape(4, SUB, quarter)
                    val[block, 2 * g + 1] = two.reshape(4, SUB, quarter)
                else:
                    low = iota((each, quarter), 0) % SUB < SUB // 2
                    val[block, 2 * full] = jnp.where(low, one, two).reshape(4, SUB, quarter)
        join()
        for step in reversed(steps):
            for place in range(4):
                dest = block_of(step, place)
                copy = remote(
                    val.at[dest], ret.at[me], send_sem.at[8], recv_sem.at[5], expert=dest
                )
                if step:
                    copy.start()
                else:
                    pl.when(spot != place)(copy.start)
        return swap

    swap_early = experts(0, lambda: None)
    across(1)

    def join_attention():
        @pl.when(me < chunks)
        def _():
            remote(
                apr.at[pl.ds(0, n - 1)],
                apr.at[pl.ds(0, n - 1)],
                send_sem.at[5],
                recv_sem.at[2],
                expert=x_side,
            ).wait_recv()
            apr[me] = aps[me]
            peaks = apr[:, :, part_w : part_w + 1]
            totals = apr[:, :, part_w + LANES // 2 : part_w + LANES // 2 + 1]
            top = jnp.max(peaks, axis=0, keepdims=True)
            scale = jnp.exp(peaks - top)
            total = jnp.sum(totals * scale, axis=0)
            joined = jnp.sum(apr[:, :, 0:part_w] * scale, axis=0)
            ares[me] = (joined / total).astype(BF16)

            def tell(step, carry):
                remote(
                    ares.at[me],
                    ares.at[me],
                    send_sem.at[7],
                    recv_sem.at[4],
                    expert=lax.rem(me + step, n),
                ).start()
                return carry

            lax.fori_loop(1, n, tell, 0)

    swap_late = experts(1, join_attention)
    ret[me] = val[me]

    spread_in = jnp.concatenate([gate_high, gate_low, code], axis=0).astype(BF16)
    spot_of = jnp.where(
        iota((LANES, n * SUB), 0) == iota((LANES, n * SUB), 1) // SUB, 1.0, 0.0
    ).astype(BF16)
    spread = jnp.dot(spread_in, spot_of, preferred_element_type=F32)
    weights = spread[: 2 * rows]
    codes_r = spread[2 * rows :]
    codes_r = jnp.concatenate([codes_r, codes_r], axis=0)
    j = iota((2 * rows, n * SUB), 1) % SUB
    mats = []
    for g in range(full):
        hit = codes_r == (g * SUB + j + 1).astype(F32)
        mats.append(jnp.where(hit, weights, 0.0).astype(BF16))
    if fold:
        hit = codes_r == (full * SUB + j % (SUB // 2) + 1).astype(F32)
        for low in (True, False):
            side = (j < SUB // 2) if low else (j >= SUB // 2)
            mats.append(jnp.where(hit & side, weights, 0.0).astype(BF16))

    @pl.when(me < chunks)
    def _():
        part = ares.at[pl.ds(0, chunks - 1)]
        remote(part, part, send_sem.at[7], recv_sem.at[4], expert=x_side).wait_recv()

    if chunks < n:

        @pl.when(me >= chunks)
        def _():
            remote(ares, ares, send_sem.at[7], recv_sem.at[4], expert=x_side).wait_recv()

    for b in range(batch):
        for g in range(per_batch):
            for c in range(parts):
                at = (b * per_batch + g) * parts + c
                attn_out[b, g * SUB : (g + 1) * SUB, c * part_w : (c + 1) * part_w] = ares[at]

    remote(xp, xp, send_sem.at[0], recv_sem.at[0], tensor=other).wait_send()
    for sem in (1, 2):
        part = xb.at[pl.ds(0, outer)]
        remote(part, part, send_sem.at[sem], recv_sem.at[0], expert=x_side).wait_send()
    for h in range(outer):
        part = xb.at[h, :, cuts[0]]
        remote(part, part, send_sem.at[2], recv_sem.at[0], expert=x_side).wait_send()
        part = xb.at[h, :, cuts[1]]
        remote(part, part, send_sem.at[1], recv_sem.at[0], expert=x_side).wait_send()
    part = xb.at[pl.ds(0, outer - 1)]
    remote(part, part, send_sem.at[3], recv_sem.at[0], expert=x_side).wait_send()
    w_swap.wait_send()
    swap_early.wait_send()
    swap_late.wait_send()

    sent = chunks - jnp.where(me < chunks, 1, 0)

    def drain(step, carry):
        remote(aps.at[0], apr.at[0], send_sem.at[5], recv_sem.at[2], expert=x_side).wait_send()
        return carry

    lax.fori_loop(0, sent, drain, 0)

    @pl.when(me < chunks)
    def _():
        def drain_result(step, carry):
            remote(
                ares.at[0], ares.at[0], send_sem.at[7], recv_sem.at[4], expert=x_side
            ).wait_send()
            return carry

        lax.fori_loop(1, n, drain_result, 0)

    part = ret.at[pl.ds(0, n - 1)]
    remote(part, part, send_sem.at[8], recv_sem.at[5], expert=x_side).wait_recv()
    lo = jnp.zeros((2 * rows, quarter), F32)
    hi = jnp.zeros((2 * rows, quarter), F32)
    for g in range(full):
        lo = lo + jnp.dot(
            mats[g], ret[:, 2 * g].reshape(n * SUB, quarter), preferred_element_type=F32
        )
        hi = hi + jnp.dot(
            mats[g], ret[:, 2 * g + 1].reshape(n * SUB, quarter), preferred_element_type=F32
        )
    if fold:
        last = ret[:, 2 * full].reshape(n * SUB, quarter)
        lo = lo + jnp.dot(mats[full], last, preferred_element_type=F32)
        hi = hi + jnp.dot(mats[full + 1], last, preferred_element_type=F32)
    ob[:, :quarter] = ((lo[:rows] + lo[rows:]) / gate_denominator).astype(BF16)
    ob[:, quarter:] = ((hi[:rows] + hi[rows:]) / gate_denominator).astype(BF16)
    o_swap = remote(ob, op, send_sem.at[9], recv_sem.at[6], tensor=other)
    o_swap.start()
    moe_out[:, mine] = ob[...]
    remote(part, part, send_sem.at[8], recv_sem.at[5], expert=x_side).wait_send()
    o_swap.wait()
    moe_out[:, theirs] = op[...]


def finish_kernel(moe, attn, moe_out, attn_out):
    moe_out[...] = moe[...]
    attn_out[...] = attn[...]


def finish(moe, attn):
    vmem = pl.BlockSpec(memory_space=pltpu.VMEM)
    return pl.pallas_call(
        finish_kernel,
        out_shape=(
            jax.ShapeDtypeStruct(moe.shape, BF16),
            jax.ShapeDtypeStruct(attn.shape, BF16),
        ),
        in_specs=[vmem, vmem],
        out_specs=(vmem, vmem),
    )(moe, attn)


def local(
    hidden_in,
    batch_len,
    expert_ids,
    gate_num,
    w_gate,
    w_up,
    w_down,
    q_latent,
    q_rope,
    kv_latent,
    kv_rope,
    ctx_len,
):
    n = lax.axis_size("expert")
    rows, width = hidden_in.shape
    topk = expert_ids.shape[1]
    capacity = min(rows, max(2, 3 * rows * topk // (2 * n)))
    rest = capacity % SUB
    full = capacity // SUB + (1 if rest > SUB // 2 else 0)
    fold = 1 if 0 < rest <= SUB // 2 else 0
    half = width // 2
    hidden = w_gate.shape[2]
    batch, heads, lat = q_latent.shape
    row_groups = batch * heads // SUB
    chunks = row_groups * min(max(1, n // row_groups), lat // LANES)
    part_w = lat * row_groups // chunks
    parts_v = 2 * full + fold
    outer = n // 4
    anywhere = pl.BlockSpec(memory_space=pl.ANY)
    vmem = pl.BlockSpec(memory_space=pltpu.VMEM)
    smem = pl.BlockSpec(memory_space=pltpu.SMEM)
    moe_out, attn_out = pl.pallas_call(
        functools.partial(kernel, n, full, fold, chunks),
        out_shape=(
            jax.ShapeDtypeStruct((rows, width), BF16),
            jax.ShapeDtypeStruct((batch, heads, lat), BF16),
        ),
        in_specs=[
            anywhere,
            smem,
            vmem,
            vmem,
            anywhere,
            anywhere,
            anywhere,
            vmem,
            vmem,
            anywhere,
            anywhere,
            smem,
        ],
        out_specs=(vmem, vmem),
        scratch_shapes=[
            pltpu.VMEM((n, rows, LANES + half), BF16),
            pltpu.VMEM((n, rows, half), BF16),
            pltpu.VMEM((2, half, hidden), BF16),
            pltpu.VMEM((2, half, hidden), BF16),
            pltpu.VMEM((2, hidden, half), BF16),
            pltpu.VMEM(kv_latent.shape, BF16),
            pltpu.VMEM(kv_rope.shape, BF16),
            pltpu.VMEM((2, n * rows, hidden), BF16),
            pltpu.VMEM((n, parts_v, SUB, half // 2), BF16),
            pltpu.VMEM((n, parts_v, SUB, half // 2), BF16),
            pltpu.VMEM((chunks, SUB, part_w + LANES), F32),
            pltpu.VMEM((n, SUB, part_w + LANES), F32),
            pltpu.VMEM((chunks, SUB, part_w), BF16),
            pltpu.VMEM((rows, half), BF16),
            pltpu.VMEM((rows, half), BF16),
            pltpu.SemaphoreType.DMA((8,)),
            pltpu.SemaphoreType.DMA((outer, 2)),
            pltpu.SemaphoreType.DMA((outer, 2)),
            pltpu.SemaphoreType.DMA((outer, 2)),
            pltpu.SemaphoreType.DMA((outer, 2)),
            pltpu.SemaphoreType.DMA((11,)),
            pltpu.SemaphoreType.DMA((10,)),
        ],
        compiler_params=pltpu.CompilerParams(
            collective_id=0, has_side_effects=True, vmem_limit_bytes=60 * 1024 * 1024
        ),
    )(
        hidden_in,
        batch_len,
        expert_ids.T,
        gate_num.T,
        w_gate,
        w_up,
        w_down,
        q_latent,
        q_rope,
        kv_latent,
        kv_rope,
        ctx_len,
    )
    return finish(moe_out, attn_out)


def solution(mesh):
    return jax.shard_map(
        local,
        mesh=mesh,
        in_specs=(
            P(("groups", "expert"), None),
            P("groups"),
            P(("groups", "expert"), None),
            P(("groups", "expert"), None),
            P("expert", None, "tensor"),
            P("expert", None, "tensor"),
            P("expert", "tensor", None),
            P("groups", "tensor", None),
            P("groups", "tensor", None),
            P("groups", "expert", None),
            P("groups", None, "expert"),
            P("groups"),
        ),
        out_specs=(P(("groups", "expert"), None), P("groups", "tensor", None)),
        check_vma=False,
    )
```
